32 devices in a mesh: dom: 8 (over y, x, core), tp: 4 (over z).
Axes of the slice: x: 2, y: 2, z: 4, core: 2. Of those that a mesh axis runs over, the one named last changes fastest.
Arguments:
- activations: bfloat16 [4, 128, 4096], P(None, 'dom', 'tp'), may hold values from -6 to 6
- norm_gain: float32 [4096], replicated, may hold values from 0.5 to 1.5
- w_query: bfloat16 [4096, 4096], P(None, 'tp'), may hold values from -0.09375 to 0.09375
- w_key: bfloat16 [4096, 1024], P(None, 'tp'), may hold values from -0.09375 to 0.09375
- value_weight: bfloat16 [4096, 1024], P(None, 'tp'), may hold values from -0.5 to 0.5
- w_output: bfloat16 [4096, 4096], P('tp'), may hold values from -0.09375 to 0.09375
- cache_keys: bfloat16 [128, 128, 1024], P('dom', None, 'tp'), may hold values from -740 to 740
- cache_values: bfloat16 [128, 128, 1024], P('dom', None, 'tp'), may hold values from -48 to 48
- tokens: int32 [4, 128], P(None, 'dom'), may hold values from 0 to 128255
- twisting_table: bfloat16 [128256], replicated, may hold values from -6 to 6
- twist_vec: float32 [4096], P('tp'), may hold values from -0.09375 to 0.09375
- previous_log_weights: float32 [128], P('dom'), may hold values from -300 to 0
- copy_counts: int32 [128], P('dom'), may hold values from 0 to 4, as said below
Outputs:
- attn_out: bfloat16 [4, 128, 4096], P(None, 'dom', 'tp')
- new_keys: bfloat16 [128, 132, 1024], P('dom', None, 'tp')
- new_values: bfloat16 [128, 132, 1024], P('dom', None, 'tp')
- out_logw: float32 [128], P('dom')
The draws below stay inside these ranges and needn't reach their ends.
Inputs may be any that keep to these rules, and one draw needn't show every extreme that they name: copy_counts sum to 128; the particles of one index of dom have together at most 64 copies, and one index has exactly that many.
All inputs are finite; a program needn't handle non-finite values.
Results may differ from the reference program's by a relative error of at most 0.012.
The reference program's roundings to bfloat16 on the way (of `normed`, `queries`, `fresh_keys`, `fresh_values`, `key_rows`, `weights` and `context`) count: a program that leaves them out, or rounds other values in their place, can miss the bound.
Values may be sent and summed in bfloat16 or wider, within the bound.
A program may use at most 128 MiB of HBM per device.

```python
import math
import jax
import jax.numpy as jnp
import numpy as np
from jax import lax

D = 4096
QH = 32
KVH = 8
HD = 128
VOCAB = 128256
STEPS = 4
PART_DEV = 16
L = 128
PARTICLES = 128
N_DOM = 8


def draw_cache_keys(key, part):
    base_key = jax.random.fold_in(jax.random.fold_in(key, 11), 0)
    width = KVH * HD
    result = jnp.clip(jax.random.normal(base_key, (PARTICLES, L, width), jnp.float32), -4.5, 4.5)
    return result.astype(jnp.bfloat16)


def draw_previous_log_weights(key, part):
    result = jax.random.uniform(jax.random.fold_in(key, 23), (PARTICLES,), jnp.float32, -8.0, 0.0)
    return result


def draw_copy_counts(key, part):
    first_key, second_key = jax.random.split(jax.random.fold_in(key, 37), 2)
    devices = PARTICLES // PART_DEV
    slots_all = 4 * PARTICLES
    heavy_device = jax.random.randint(first_key, (), 0, devices)
    shuffle = jax.random.permutation(second_key, slots_all)
    owner_device = jnp.arange(slots_all, dtype=jnp.int32) // (4 * PART_DEV)
    lighter = (owner_device[shuffle] != heavy_device).astype(jnp.int32)
    running = jnp.cumsum(lighter)
    needed = (devices - 4) * PART_DEV
    picked_order = ((lighter == 1) & (running <= needed)).astype(jnp.int32)
    picked = jnp.zeros((slots_all,), jnp.int32).at[shuffle].set(picked_order)
    picked = jnp.maximum(picked, (owner_device == heavy_device).astype(jnp.int32))
    return jnp.sum(picked.reshape(PARTICLES, 4), 1).astype(jnp.int32)


def set_ends(values, stream_key, smallest, top_value):
    dims = values.shape
    place = [jax.random.randint(jax.random.fold_in(stream_key, axis), (), 0, dims[axis]) for axis in range(len(dims))]
    values = values.at[tuple(place)].set(smallest)
    longest = dims.index(max(dims))
    place[longest] = (place[longest] + 1) % dims[longest]
    return values.at[tuple(place)].set(top_value)


def block_levels(key, extent, cuts, smallest, top_value):
    gain = 1.0
    for dim, shards_of in cuts:
        heights = jax.random.uniform(jax.random.fold_in(jax.random.fold_in(key, 6), dim), (shards_of,), jnp.float32, smallest / len(cuts), top_value / len(cuts))
        gain = gain * jnp.repeat(jnp.exp(heights), extent[dim] // shards_of).reshape((-1,) + (1,) * (len(extent) - 1 - dim))
    return gain


def wide_ids(own_key, shape, number_of, lean):
    loads = [min(1 << octave, number_of + 1 - (1 << octave)) * (1 << 20) // math.isqrt((1 << octave) ** lean) + 1 for octave in range((number_of + 1).bit_length()) if 1 << octave <= number_of]
    scale = 1 + sum(loads) // (1 << 30)
    listing = np.cumsum(np.array([max(1, weight // scale) for weight in loads]))
    lot = jax.random.randint(jax.random.fold_in(own_key, 1), shape, 0, int(listing[len(loads) - 1]))
    start = jnp.left_shift(1, jnp.searchsorted(jnp.asarray(listing, jnp.int32), lot, side="right").astype(jnp.int32))
    rank = start - 1 + jax.random.randint(jax.random.fold_in(own_key, 4), shape, 0, 1 << 30) % jnp.minimum(start, number_of + 1 - start)
    return jax.random.permutation(jax.random.fold_in(own_key, 2), number_of)[rank].astype(jnp.int32)


def normal_values(key, shape, scale, reach, cuts=(), kind=jnp.bfloat16):
    values = jax.random.normal(key, shape, jnp.float32) * scale
    if len(cuts) > 0:
        values = block_levels(key, shape, cuts, -0.22, 0.18) * values
    return jnp.clip(values, min=-reach, max=reach).astype(kind)


def setup_inputs(seed: int = 0) -> dict:
    keys = jax.random.split(jax.random.key(seed), 14)
    return {
        "activations": normal_values(keys[0], (STEPS, PARTICLES, D), 1.0, 6.0, ((1, 8), (2, 4))),
        "norm_gain": jnp.clip(1.0 + 0.1 * jax.random.normal(keys[1], (D,), jnp.float32), 0.5, 1.5),
        "w_query": normal_values(keys[2], (D, QH * HD), D ** -0.5, 0.09375, ((1, 4),)),
        "w_key": normal_values(keys[3], (D, KVH * HD), D ** -0.5, 0.09375, ((1, 4),)),
        "value_weight": normal_values(keys[4], (D, KVH * HD), (D // 32) ** -0.5, 0.5, ((1, 4),)),
        "w_output": normal_values(keys[5], (QH * HD, D), (QH * HD) ** -0.5, 0.09375, ((0, 4),)),
        "cache_keys": draw_cache_keys(jax.random.fold_in(keys[13], 71), 0),
        "cache_values": normal_values(keys[7], (PARTICLES, L, KVH * HD), 8.0, 48.0, ((0, 8), (2, 4))),
        "tokens": set_ends(wide_ids(keys[8], (STEPS, PARTICLES), VOCAB, 2), jax.random.fold_in(keys[8], 3), 0, VOCAB - 1).astype(jnp.int32),
        "twisting_table": normal_values(keys[9], (VOCAB,), 1.0, 6.0),
        "twist_vec": normal_values(keys[10], (D,), D ** -0.5, 0.09375, ((0, 4),), jnp.float32),
        "previous_log_weights": draw_previous_log_weights(jax.random.fold_in(keys[13], 71), 0),
        "copy_counts": draw_copy_counts(jax.random.fold_in(keys[13], 71), 0),
    }


def rotate(tensor, positions):
    middle = tensor.shape[-1] // 2
    frequency = 500000.0 ** (-2.0 * jnp.arange(middle, dtype=jnp.float32) / tensor.shape[-1])
    angles = positions[:, None] * frequency[None, :]
    cosine = jnp.cos(angles)[:, None, None, :]
    sine_part = jnp.sin(angles)[:, None, None, :]
    lower_half = tensor[..., :middle]
    upper_half = tensor[..., middle:]
    return jnp.concatenate([lower_half * cosine - upper_half * sine_part, upper_half * cosine + lower_half * sine_part], -1)

def reference(activations, norm_gain, w_query, w_key, value_weight, w_output, cache_keys, cache_values, tokens, twisting_table, twist_vec, previous_log_weights, copy_counts):
    inputs = activations.astype(jnp.float32)
    normed = (inputs * lax.rsqrt(lax.optimization_barrier(jnp.mean(inputs * inputs, -1, keepdims=True)) + 1e-05) * norm_gain).astype(jnp.bfloat16)
    flat_rows = normed.reshape(STEPS * PARTICLES, D)
    positions = (L + jnp.arange(STEPS, dtype=jnp.int32)).astype(jnp.float32)
    queries = jnp.dot(flat_rows, w_query, preferred_element_type=jnp.float32).reshape(STEPS, PARTICLES, QH, HD)
    queries = rotate(queries, positions).astype(jnp.bfloat16)
    fresh_keys = jnp.dot(flat_rows, w_key, preferred_element_type=jnp.float32).reshape(STEPS, PARTICLES, KVH, HD)
    fresh_keys = rotate(fresh_keys, positions).astype(jnp.bfloat16).reshape(STEPS, PARTICLES, KVH * HD)
    fresh_values = jnp.dot(flat_rows, value_weight, preferred_element_type=jnp.float32).astype(jnp.bfloat16).reshape(STEPS, PARTICLES, KVH * HD)
    key_rows = jnp.concatenate([cache_keys, jnp.transpose(fresh_keys, (1, 0, 2))], 1)
    value_rows = jnp.concatenate([cache_values, jnp.transpose(fresh_values, (1, 0, 2))], 1)
    key_span = L + STEPS
    group_size = QH // KVH
    query_heads = queries.reshape(STEPS, PARTICLES, KVH, group_size, HD).astype(jnp.float32)
    key_heads = key_rows.reshape(PARTICLES, key_span, KVH, HD).astype(jnp.float32)
    value_heads = value_rows.reshape(PARTICLES, key_span, KVH, HD).astype(jnp.float32)
    scores = jnp.einsum('snkgd,nlkd->snkgl', query_heads, key_heads) / HD ** 0.5
    allowed = jnp.arange(key_span, dtype=jnp.int32)[None, :] <= (L + jnp.arange(STEPS, dtype=jnp.int32))[:, None]
    allowed = allowed[:, None, None, None, :]
    masked = jnp.where(allowed, scores, -jnp.inf)
    highest = lax.optimization_barrier(jnp.max(masked, -1, keepdims=True))
    exponent = jnp.exp(masked - highest)
    weights = (exponent / lax.optimization_barrier(jnp.sum(exponent, -1, keepdims=True))).astype(jnp.bfloat16)
    context = jnp.einsum('snkgl,nlkd->snkgd', weights.astype(jnp.float32), value_heads).astype(jnp.bfloat16)
    context = context.reshape(STEPS * PARTICLES, QH * HD)
    head_mix = jnp.dot(context, w_output, preferred_element_type=jnp.float32).reshape(STEPS, PARTICLES, D)
    attn_out = head_mix.astype(jnp.bfloat16)
    summed = inputs + head_mix
    twisting_score = lax.optimization_barrier(jnp.sum(summed * twist_vec, -1)) / jnp.sqrt(lax.optimization_barrier(jnp.mean(summed * summed, -1)) + 1e-06)
    token_reward = twisting_table[tokens].astype(jnp.float32)
    particle_log_weight = previous_log_weights + lax.optimization_barrier(jnp.sum(token_reward + twisting_score, 0))
    largest = jnp.max(particle_log_weight)
    out_logw = particle_log_weight - (largest + jnp.log(jnp.sum(jnp.exp(particle_log_weight - largest))))
    copy_ends = jnp.cumsum(copy_counts).astype(jnp.int32)
    new_slot = jnp.arange(PARTICLES, dtype=jnp.int32)
    owner_index = new_slot // PART_DEV
    local_slot = new_slot % PART_DEV
    copy_rank = local_slot * N_DOM + owner_index
    ancestor = lax.optimization_barrier(jnp.sum((copy_ends[None, :] <= copy_rank[:, None]).astype(jnp.int32), 1)).astype(jnp.int32)
    new_keys = key_rows[ancestor]
    new_values = value_rows[ancestor]
    return (attn_out, new_keys, new_values, out_logw)
```

```python
import jax
import jax.numpy as jnp
from jax import lax
from jax.sharding import PartitionSpec as P

D = 4096
HD = 128


def entering(part, axis, combine, identity):
    place = lax.axis_index(axis)
    gathered = lax.all_gather(part, axis)
    state = jnp.zeros_like(part) + jnp.asarray(identity, part.dtype)

    def one(lap, state):
        return combine(state, lax.dynamic_index_in_dim(gathered, lap, 0, False))

    return lax.fori_loop(0, place, one, state)


def rotate(tensor, positions):
    middle = tensor.shape[-1] // 2
    frequency = 500000.0 ** (-2.0 * jnp.arange(middle, dtype=jnp.float32) / tensor.shape[-1])
    angles = positions[:, None] * frequency[None, :]
    cosine = jnp.cos(angles)[:, None, None, :]
    sine_part = jnp.sin(angles)[:, None, None, :]
    lower_half = tensor[..., :middle]
    upper_half = tensor[..., middle:]
    return jnp.concatenate(
        [
            lower_half * cosine - upper_half * sine_part,
            upper_half * cosine + lower_half * sine_part,
        ],
        -1,
    )


def add_counts(former, latter):
    return former + latter


def local(
    activations,
    norm_gain,
    w_query,
    w_key,
    value_weight,
    w_output,
    cache_keys,
    cache_values,
    tokens,
    twisting_table,
    twist_vec,
    previous_log_weights,
    copy_counts,
):
    step_count = activations.shape[0]
    particle_count = activations.shape[1]
    span_old = cache_keys.shape[1]
    dom_size = lax.axis_size("dom")
    kv_local = w_key.shape[1] // HD
    q_local = w_query.shape[1] // HD
    group_size = q_local // kv_local
    all_counts = lax.all_gather(copy_counts, "dom", axis=0, tiled=True)
    copy_ends = jnp.cumsum(all_counts)
    ranks = jnp.arange(particle_count, dtype=jnp.int32) * dom_size + lax.axis_index("dom")
    ancestor = jnp.sum((copy_ends[None, :] <= ranks[:, None]).astype(jnp.int32), 1)
    all_keys = lax.all_gather(cache_keys, "dom", axis=0, tiled=True)
    all_values = lax.all_gather(cache_values, "dom", axis=0, tiled=True)

    gathered = lax.all_gather(activations, "tp", axis=2, tiled=True)
    inputs = gathered.astype(jnp.float32)
    normed = (
        inputs * lax.rsqrt(jnp.mean(inputs * inputs, -1, keepdims=True) + 1e-05) * norm_gain
    ).astype(jnp.bfloat16)
    flat_rows = normed.reshape(step_count * particle_count, D)
    positions = (span_old + jnp.arange(step_count, dtype=jnp.int32)).astype(jnp.float32)
    queries = jnp.dot(flat_rows, w_query, preferred_element_type=jnp.float32).reshape(
        step_count, particle_count, q_local, HD
    )
    queries = rotate(queries, positions).astype(jnp.bfloat16)
    fresh_keys = jnp.dot(flat_rows, w_key, preferred_element_type=jnp.float32).reshape(
        step_count, particle_count, kv_local, HD
    )
    fresh_keys = (
        rotate(fresh_keys, positions)
        .astype(jnp.bfloat16)
        .reshape(step_count, particle_count, kv_local * HD)
    )
    fresh_values = jnp.dot(flat_rows, value_weight, preferred_element_type=jnp.float32).astype(
        jnp.bfloat16
    )
    fresh_values = fresh_values.reshape(step_count, particle_count, kv_local * HD)
    fresh_keys = jnp.transpose(fresh_keys, (1, 0, 2))
    fresh_values = jnp.transpose(fresh_values, (1, 0, 2))
    key_rows = jnp.concatenate([cache_keys, fresh_keys], 1)
    value_rows = jnp.concatenate([cache_values, fresh_values], 1)
    key_span = span_old + step_count
    query_heads = queries.reshape(step_count, particle_count, kv_local, group_size, HD)
    key_heads = key_rows.reshape(particle_count, key_span, kv_local, HD)
    value_heads = value_rows.reshape(particle_count, key_span, kv_local, HD)
    scores = (
        jnp.einsum("snkgd,nlkd->snkgl", query_heads, key_heads, preferred_element_type=jnp.float32)
        / HD**0.5
    )
    allowed = (
        jnp.arange(key_span, dtype=jnp.int32)[None, :]
        <= (span_old + jnp.arange(step_count, dtype=jnp.int32))[:, None]
    )
    allowed = allowed[:, None, None, None, :]
    masked = jnp.where(allowed, scores, -jnp.inf)
    highest = jnp.max(masked, -1, keepdims=True)
    exponent = jnp.exp(masked - highest)
    weights = (exponent / jnp.sum(exponent, -1, keepdims=True)).astype(jnp.bfloat16)
    context = jnp.einsum(
        "snkgl,nlkd->snkgd", weights, value_heads, preferred_element_type=jnp.float32
    ).astype(jnp.bfloat16)
    context = context.reshape(step_count * particle_count, q_local * HD)
    partial_value = jnp.dot(context, w_output, preferred_element_type=jnp.float32).reshape(
        step_count, particle_count, D
    )
    head_mix = lax.psum_scatter(partial_value, "tp", scatter_dimension=2, tiled=True)
    attn_out = head_mix.astype(jnp.bfloat16)
    summed = activations.astype(jnp.float32) + head_mix
    aligned, energy = lax.psum(
        (jnp.sum(summed * twist_vec, -1), jnp.sum(summed * summed, -1)), "tp"
    )
    twisting_score = aligned / jnp.sqrt(energy / D + 1e-06)
    token_reward = twisting_table[tokens].astype(jnp.float32)
    particle_log_weight = previous_log_weights + jnp.sum(token_reward + twisting_score, 0)
    largest = lax.pmax(jnp.max(particle_log_weight), "dom")
    mass_total = lax.psum(jnp.sum(jnp.exp(particle_log_weight - largest)), "dom")
    out_logw = particle_log_weight - (largest + jnp.log(mass_total))
    fresh = lax.all_gather(
        jnp.concatenate([fresh_keys, fresh_values], 2), "dom", axis=0, tiled=True
    )[ancestor]
    width = fresh_keys.shape[2]
    new_keys = jnp.concatenate([all_keys[ancestor], fresh[..., :width]], 1)
    new_values = jnp.concatenate([all_values[ancestor], fresh[..., width:]], 1)
    return (attn_out, new_keys, new_values, out_logw)


def solution(mesh):
    return jax.shard_map(
        local,
        mesh=mesh,
        in_specs=(
            P(None, "dom", "tp"),
            P(),
            P(None, "tp"),
            P(None, "tp"),
            P(None, "tp"),
            P("tp", None),
            P("dom", None, "tp"),
            P("dom", None, "tp"),
            P(None, "dom"),
            P(),
            P("tp"),
            P("dom"),
            P("dom"),
        ),
        out_specs=(P(None, "dom", "tp"), P("dom", None, "tp"), P("dom", None, "tp"), P("dom")),
        check_vma=False,
    )
```

```python
import functools

import jax
import jax.numpy as jnp
import numpy as np
from jax import lax
from jax.experimental import pallas as pl
from jax.experimental.pallas import tpu as pltpu
from jax.sharding import PartitionSpec as P

D = 4096
HD = 128


def rotate(tensor, positions):
    middle = tensor.shape[-1] // 2
    frequency = 500000.0 ** (-2.0 * jnp.arange(middle, dtype=jnp.float32) / tensor.shape[-1])
    angles = positions[:, None] * frequency[None, :]
    cosine = jnp.cos(angles)[:, None, None, :]
    sine_part = jnp.sin(angles)[:, None, None, :]
    lower_half = tensor[..., :middle]
    upper_half = tensor[..., middle:]
    return jnp.concatenate(
        [
            lower_half * cosine - upper_half * sine_part,
            upper_half * cosine + lower_half * sine_part,
        ],
        -1,
    )


def local(
    activations,
    norm_gain,
    w_query,
    w_key,
    value_weight,
    w_output,
    cache_keys,
    cache_values,
    tokens,
    twisting_table,
    twist_vec,
    previous_log_weights,
    copy_counts,
):
    step_count = activations.shape[0]
    particle_count = activations.shape[1]
    span_old = cache_keys.shape[1]
    dom_size = lax.axis_size("dom")
    kv_local = w_key.shape[1] // HD
    q_local = w_query.shape[1] // HD
    group_size = q_local // kv_local
    all_counts = lax.all_gather(copy_counts, "dom", axis=0, tiled=True)
    copy_ends = jnp.cumsum(all_counts)
    ranks = jnp.arange(particle_count, dtype=jnp.int32) * dom_size + lax.axis_index("dom")
    ancestor = jnp.sum((copy_ends[None, :] <= ranks[:, None]).astype(jnp.int32), 1)
    all_keys = lax.all_gather(cache_keys, "dom", axis=0, tiled=True)
    all_values = lax.all_gather(cache_values, "dom", axis=0, tiled=True)

    gathered = lax.all_gather(activations, "tp", axis=2, tiled=True)
    inputs = gathered.astype(jnp.float32)
    normed = (
        inputs * lax.rsqrt(jnp.mean(inputs * inputs, -1, keepdims=True) + 1e-05) * norm_gain
    ).astype(jnp.bfloat16)
    flat_rows = normed.reshape(step_count * particle_count, D)
    positions = (span_old + jnp.arange(step_count, dtype=jnp.int32)).astype(jnp.float32)
    queries = jnp.dot(flat_rows, w_query, preferred_element_type=jnp.float32).reshape(
        step_count, particle_count, q_local, HD
    )
    queries = rotate(queries, positions).astype(jnp.bfloat16)
    fresh_keys = jnp.dot(flat_rows, w_key, preferred_element_type=jnp.float32).reshape(
        step_count, particle_count, kv_local, HD
    )
    fresh_keys = (
        rotate(fresh_keys, positions)
        .astype(jnp.bfloat16)
        .reshape(step_count, particle_count, kv_local * HD)
    )
    fresh_values = jnp.dot(flat_rows, value_weight, preferred_element_type=jnp.float32).astype(
        jnp.bfloat16
    )
    fresh_values = fresh_values.reshape(step_count, particle_count, kv_local * HD)
    fresh_keys = jnp.transpose(fresh_keys, (1, 0, 2))
    fresh_values = jnp.transpose(fresh_values, (1, 0, 2))
    key_rows = jnp.concatenate([cache_keys, fresh_keys], 1)
    value_rows = jnp.concatenate([cache_values, fresh_values], 1)
    key_span = span_old + step_count
    query_heads = queries.reshape(step_count, particle_count, kv_local, group_size, HD)
    key_heads = key_rows.reshape(particle_count, key_span, kv_local, HD)
    value_heads = value_rows.reshape(particle_count, key_span, kv_local, HD)
    scores = (
        jnp.einsum("snkgd,nlkd->snkgl", query_heads, key_heads, preferred_element_type=jnp.float32)
        / HD**0.5
    )
    allowed = (
        jnp.arange(key_span, dtype=jnp.int32)[None, :]
        <= (span_old + jnp.arange(step_count, dtype=jnp.int32))[:, None]
    )
    allowed = allowed[:, None, None, None, :]
    masked = jnp.where(allowed, scores, -jnp.inf)
    highest = jnp.max(masked, -1, keepdims=True)
    exponent = jnp.exp(masked - highest)
    weights = (exponent / jnp.sum(exponent, -1, keepdims=True)).astype(jnp.bfloat16)
    context = jnp.einsum(
        "snkgl,nlkd->snkgd", weights, value_heads, preferred_element_type=jnp.float32
    ).astype(jnp.bfloat16)
    context = context.reshape(step_count * particle_count, q_local * HD)
    partial_value = jnp.dot(context, w_output, preferred_element_type=jnp.float32).reshape(
        step_count, particle_count, D
    )
    head_mix = lax.psum_scatter(partial_value, "tp", scatter_dimension=2, tiled=True)
    attn_out = head_mix.astype(jnp.bfloat16)
    summed = activations.astype(jnp.float32) + head_mix
    aligned, energy = lax.psum(
        (jnp.sum(summed * twist_vec, -1), jnp.sum(summed * summed, -1)), "tp"
    )
    twisting_score = aligned / jnp.sqrt(energy / D + 1e-06)
    token_reward = twisting_table[tokens].astype(jnp.float32)
    particle_log_weight = previous_log_weights + jnp.sum(token_reward + twisting_score, 0)
    largest = lax.pmax(jnp.max(particle_log_weight), "dom")
    mass_total = lax.psum(jnp.sum(jnp.exp(particle_log_weight - largest)), "dom")
    out_logw = particle_log_weight - (largest + jnp.log(mass_total))
    fresh = lax.all_gather(
        jnp.concatenate([fresh_keys, fresh_values], 2), "dom", axis=0, tiled=True
    )[ancestor]
    width = fresh_keys.shape[2]
    new_keys = jnp.concatenate([all_keys[ancestor], fresh[..., :width]], 1)
    new_values = jnp.concatenate([all_values[ancestor], fresh[..., width:]], 1)
    return (attn_out, new_keys, new_values, out_logw)


MESH = pl.DeviceIdType.MESH


def layer_kernel(
    steps, parts, doms, tps,
    act, gain, wq, wk, wv, wo, ck, cv, reward, twist, prev, counts, cosine, sine,
    attn_out, all_k, all_v, fresh_sel, out_lw, anc_out,
    act_all, wq_v, wk_v, wv_v, wo_v, ck_v, cv_v, qs, cx, sc1, ctx_b, fresh, fresh_all,
    rs_send, rs_recv, sc_all, lw_all, cnt_all,
    loc, tp_send, tp_recv, dom_send, dom_recv, blk_send, blk_recv,
):
    f32, bf16 = jnp.float32, jnp.bfloat16
    me_d = lax.axis_index("dom")
    me_t = lax.axis_index("tp")
    rows, width = act.shape
    half = parts // 2
    kvw = wk.shape[1]
    groups = kvw // HD
    per = wq.shape[1] // kvw
    pack = steps * per
    c = me_d % 2
    x = (me_d // 2) % 2
    y = me_d // 4
    sib = me_d + 1 - 2 * c
    xn = me_d + 2 - 4 * x
    yn = me_d + 4 - 8 * y
    dn = xn + 4 - 8 * y

    barrier = pltpu.get_barrier_semaphore()
    for k in range(1, tps):
        pl.semaphore_signal(
            barrier, inc=1, device_id=(me_d, (me_t + k) % tps), device_id_type=MESH
        )
    for k in range(1, doms):
        pl.semaphore_signal(
            barrier, inc=1, device_id=((me_d + k) % doms, me_t), device_id_type=MESH
        )

    def fetch(i, src, dst):
        copy = pltpu.make_async_copy(src, dst, loc.at[i])
        copy.start()
        return copy

    own_act = fetch(0, act, act_all.at[me_t])
    load_q = fetch(1, wq, wq_v)
    load_k = fetch(2, wk, wk_v)
    load_v = fetch(3, wv, wv_v)
    load_ck = fetch(4, ck, ck_v)
    load_cv = fetch(5, cv, cv_v)
    load_o = fetch(6, wo, wo_v)

    cnt_all[me_d] = jnp.broadcast_to(counts[...], cnt_all.shape[1:])
    pl.semaphore_wait(barrier, tps + doms - 2)

    def tp_push(base, k, src, dst):
        copy = pltpu.make_async_remote_copy(
            src_ref=src, dst_ref=dst, send_sem=tp_send.at[base + k - 1],
            recv_sem=tp_recv.at[base + k - 1],
            device_id=(me_d, (me_t + k) % tps), device_id_type=MESH,
        )
        copy.start()
        return copy

    def dom_push(base, k, src, dst):
        copy = pltpu.make_async_remote_copy(
            src_ref=src, dst_ref=dst, send_sem=dom_send.at[base + k - 1],
            recv_sem=dom_recv.at[base + k - 1],
            device_id=((me_d + k) % doms, me_t), device_id_type=MESH,
        )
        copy.start()
        return copy

    acts = [tp_push(0, k, act, act_all.at[me_t]) for k in range(1, tps)]

    def piece(kind, to, which, h, slot, own):
        dst = (all_k, all_v)[which].at[slot, pl.ds(h * half, half)]
        src = (ck, cv)[which].at[pl.ds(h * half, half)] if own else dst
        i = kind * 4 + h * 2 + which
        copy = pltpu.make_async_remote_copy(
            src_ref=src, dst_ref=dst, send_sem=blk_send.at[i], recv_sem=blk_recv.at[i],
            device_id=(to, me_t), device_id_type=MESH,
        )
        copy.start()
        return copy

    moves = {}
    for h, kind, to in ((0, 0, xn), (1, 1, yn), (1, 0, xn), (0, 1, yn)):
        for which in range(2):
            moves[kind, h, which] = piece(kind, to, which, h, me_d, True)
    cnts = [dom_push(0, k, cnt_all.at[me_d], cnt_all.at[me_d]) for k in range(1, doms)]
    for h in range(2):
        for which in range(2):
            moves[3, h, which] = piece(3, sib, which, h, me_d, True)

    own_act.wait()
    for copy in acts:
        copy.wait()
    square = jnp.zeros((rows, 1), f32)
    for t in range(tps):
        u = act_all[t].astype(f32)
        square = square + jnp.sum(u * u, -1, keepdims=True)
    inv = lax.rsqrt(square / (width * tps) + 1e-05)
    normed = []
    for t in range(tps):
        u = act_all[t].astype(f32)
        normed.append((u * inv * gain[:, t * width : (t + 1) * width]).astype(bf16))

    def project(w):
        total = None
        for t in range(tps):
            part = jnp.dot(
                normed[t], w[t * width : (t + 1) * width, :], preferred_element_type=f32
            )
            total = part if total is None else total + part
        return total

    cos_t, sin_t = cosine[...], sine[...]

    def turn(u):
        return u * cos_t + pltpu.roll(u, HD // 2, 1) * sin_t

    load_k.wait()
    load_v.wait()
    keys = project(wk_v)
    for g in range(groups):
        fresh[:, g * HD : (g + 1) * HD] = turn(keys[:, g * HD : (g + 1) * HD]).astype(bf16)
    fresh[:, kvw:] = project(wv_v).astype(bf16)
    fresh_all[me_d] = fresh[...]
    news = [dom_push(doms - 1, k, fresh, fresh_all.at[me_d]) for k in range(1, doms)]
    load_q.wait()
    query = project(wq_v)
    for h in range(groups * per):
        g, j = h // per, h % per
        turned = turn(query[:, h * HD : (h + 1) * HD])
        for s in range(steps):
            qs[g, :, s * per + j, :] = turned[s * parts : (s + 1) * parts]
    load_ck.wait()
    load_cv.wait()
    put_k = fetch(7, ck_v, all_k.at[me_d])
    put_v = fetch(8, cv_v, all_v.at[me_d])

    lines = parts * pack
    row = lax.broadcasted_iota(jnp.int32, (lines, rows), 0)
    col = lax.broadcasted_iota(jnp.int32, (lines, rows), 1)
    allowed = (row // pack == col % parts) & (col // parts <= (row % pack) // per)
    scale = HD**0.5
    for g in range(groups):
        lanes = slice(g * HD, (g + 1) * HD)
        qg = qs[g].reshape(lines, HD).astype(bf16)
        for n in range(parts):
            sc1[g, n * pack : (n + 1) * pack, :] = lax.dot_general(
                qg[n * pack : (n + 1) * pack], ck_v[n, :, lanes],
                (((1,), (1,)), ((), ())), preferred_element_type=f32,
            )
        near = lax.dot_general(
            qg, fresh[:, lanes], (((1,), (1,)), ((), ())), preferred_element_type=f32
        )
        near = jnp.where(allowed, near / scale, -jnp.inf)
        far = sc1[g] / scale
        top = jnp.maximum(
            jnp.max(far, -1, keepdims=True), jnp.max(near, -1, keepdims=True)
        )
        far = jnp.exp(far - top)
        near = jnp.exp(near - top)
        mass = jnp.sum(far, -1, keepdims=True) + jnp.sum(near, -1, keepdims=True)
        far = (far / mass).astype(bf16)
        near = (near / mass).astype(bf16)
        extra = jnp.dot(
            near, fresh[:, kvw + g * HD : kvw + (g + 1) * HD], preferred_element_type=f32
        )
        for n in range(parts):
            span = slice(n * pack, (n + 1) * pack)
            cx[g, n] = extra[span] + jnp.dot(
                far[span], cv_v[n, :, lanes], preferred_element_type=f32
            )
    for h in range(groups * per):
        g, j = h // per, h % per
        for s in range(steps):
            ctx_b[s * parts : (s + 1) * parts, h * HD : (h + 1) * HD] = cx[
                g, :, s * per + j, :
            ].astype(bf16)
    load_o.wait()

    def mix(p):
        return jnp.dot(
            ctx_b[...], wo_v[:, pl.ds(pl.multiple_of(p * width, HD), width)],
            preferred_element_type=f32,
        )

    sums = []
    for k in range(1, tps):
        rs_send[k - 1] = mix((me_t + k) % tps)
        sums.append(tp_push(tps - 1, k, rs_send.at[k - 1], rs_recv.at[k - 1]))
    head = mix(me_t)
    for k in range(1, tps):
        sums[k - 1].wait()
        head = head + rs_recv[k - 1]
    attn_out[...] = head.astype(bf16)
    summed = act_all[me_t].astype(f32) + head
    along = jnp.sum(summed * twist[...], -1, keepdims=True)
    energy = jnp.sum(summed * summed, -1, keepdims=True)
    lane = lax.broadcasted_iota(jnp.int32, (rows, HD), 1)
    sc_all[me_t] = jnp.where(lane < HD // 2, along, energy)
    scores = [
        tp_push(2 * (tps - 1), k, sc_all.at[me_t], sc_all.at[me_t]) for k in range(1, tps)
    ]
    for copy in scores:
        copy.wait()
    both = sc_all[0]
    for t in range(1, tps):
        both = both + sc_all[t]
    score = reward[...] + both[:, :1] / jnp.sqrt(both[:, HD - 1 :] / (width * tps) + 1e-06)
    total = score[:parts]
    for s in range(1, steps):
        total = total + score[s * parts : (s + 1) * parts]
    mine = jnp.broadcast_to(prev[...] + total, (parts, HD))
    lw_all[me_d] = mine
    lws = [
        dom_push(2 * (doms - 1), k, lw_all.at[me_d], lw_all.at[me_d]) for k in range(1, doms)
    ]

    def done(kind, h):
        for which in range(2):
            moves[kind, h, which].wait_recv()

    def relay(kind, to, h, slot):
        for which in range(2):
            moves[kind, h, which] = piece(kind, to, which, h, slot, False)

    done(0, 0)
    relay(2, yn, 0, xn)
    relay(4, sib, 0, xn)
    done(1, 1)
    relay(6, xn, 1, yn)
    relay(5, sib, 1, yn)
    done(0, 1)
    relay(4, sib, 1, xn)
    done(1, 0)
    relay(5, sib, 0, yn)

    for copy in cnts:
        copy.wait()
    for copy in news:
        copy.wait()
    whole = parts * doms
    number = cnt_all[...].reshape(whole, HD).astype(bf16)
    lower = lax.broadcasted_iota(jnp.int32, (whole, whole), 0)
    upper = lax.broadcasted_iota(jnp.int32, (whole, whole), 1)
    ends = jnp.dot(
        (upper <= lower).astype(f32).astype(bf16), number, preferred_element_type=f32
    )
    slot = lax.broadcasted_iota(jnp.int32, (whole, HD), 1)

    def ancestor(place):
        rank = (place * doms + me_d).astype(f32)
        return jnp.sum((ends <= rank).astype(f32), 0, keepdims=True).astype(jnp.int32)

    anc_out[...] = jnp.broadcast_to(ancestor(slot), anc_out.shape)
    lanes = lax.broadcasted_iota(jnp.int32, (1, HD), 1)
    wide = ancestor(slot // 8)
    target = (wide // parts) * rows + (lanes % 8) * parts + wide % parts
    target = jnp.where(lanes % 8 < steps, target, -1)
    index = lax.broadcasted_iota(jnp.int32, (doms * rows, HD), 0)
    pick = (index == target).astype(f32).astype(bf16)
    fresh_sel[...] = lax.dot_general(
        pick, fresh_all[...].reshape(doms * rows, 2 * kvw),
        (((0,), (0,)), ((), ())), preferred_element_type=f32,
    ).astype(bf16)

    for copy in lws:
        copy.wait()
    largest = jnp.max(lw_all[...], (0, 1), keepdims=True)[0]
    mass = jnp.sum(jnp.exp(lw_all[...] - largest[None]), (0, 1), keepdims=True)[0]
    out_lw[...] = mine - (largest + jnp.log(mass))

    done(2, 0)
    relay_d0 = [piece(7, sib, which, 0, dn, False) for which in range(2)]
    done(6, 1)
    relay_d1 = [piece(7, sib, which, 1, dn, False) for which in range(2)]
    for kind in (3, 4, 5):
        for h in range(2):
            done(kind, h)
    for copy in moves.values():
        copy.wait_send()
    for copy in relay_d0 + relay_d1:
        copy.wait()
    put_k.wait()
    put_v.wait()


def select_kernel(parts, steps, anc, fresh_sel, all_k, all_v, new_k, new_v, sem):
    span = all_k.shape[2]
    width = all_k.shape[3]
    copies = []
    for i in range(parts):
        a = anc[i]
        d, n = a // parts, a % parts
        for which, (src, dst) in enumerate(((all_k, new_k), (all_v, new_v))):
            copy = pltpu.make_async_copy(
                src.at[d, n], dst.at[i, pl.ds(0, span)], sem.at[2 * i + which]
            )
            copy.start()
            copies.append(copy)
    for i in range(parts):
        new_k[i, span:, :] = fresh_sel[i * 8 : i * 8 + steps, :width]
        new_v[i, span:, :] = fresh_sel[i * 8 : i * 8 + steps, width:]
    for copy in copies:
        copy.wait()


def fused(
    activations, norm_gain, w_query, w_key, value_weight, w_output, cache_keys, cache_values,
    tokens, twisting_table, twist_vec, previous_log_weights, copy_counts,
):
    f32, bf16 = jnp.float32, jnp.bfloat16
    steps, parts, width = activations.shape
    rows = steps * parts
    span = cache_keys.shape[1]
    kvw = w_key.shape[1]
    qw = w_query.shape[1]
    groups = kvw // HD
    pack = steps * (qw // kvw)
    doms = lax.axis_size("dom")
    tps = lax.axis_size("tp")
    middle = HD // 2
    angles = (span + np.arange(rows) // parts)[:, None] * (
        500000.0 ** (-2.0 * np.arange(middle) / HD)
    )
    cosine = np.concatenate([np.cos(angles)] * 2, 1).astype(np.float32)
    sine = np.concatenate([-np.sin(angles), np.sin(angles)], 1).astype(np.float32)
    reward = twisting_table[tokens.reshape(rows)].astype(f32).reshape(rows, 1)
    vmem = pl.BlockSpec(memory_space=pltpu.VMEM)
    hbm = pl.BlockSpec(memory_space=pl.ANY)
    block = jax.ShapeDtypeStruct((doms,) + cache_keys.shape, bf16)
    attn, all_k, all_v, fresh_sel, out_lw, anc = pl.pallas_call(
        functools.partial(layer_kernel, steps, parts, doms, tps),
        out_shape=(
            jax.ShapeDtypeStruct((rows, width), bf16), block, block,
            jax.ShapeDtypeStruct((HD, 2 * kvw), bf16),
            jax.ShapeDtypeStruct((parts, HD), f32),
            jax.ShapeDtypeStruct((8, HD), jnp.int32),
        ),
        in_specs=[hbm, vmem] + [hbm] * 6 + [vmem] * 6,
        out_specs=(vmem, hbm, hbm, vmem, vmem, vmem),
        scratch_shapes=[
            pltpu.VMEM((tps, rows, width), bf16),
            pltpu.VMEM(w_query.shape, bf16),
            pltpu.VMEM(w_key.shape, bf16),
            pltpu.VMEM(value_weight.shape, bf16),
            pltpu.VMEM(w_output.shape, bf16),
            pltpu.VMEM(cache_keys.shape, bf16),
            pltpu.VMEM(cache_values.shape, bf16),
            pltpu.VMEM((groups, parts, pack, HD), f32),
            pltpu.VMEM((groups, parts, pack, HD), f32),
            pltpu.VMEM((groups, parts * pack, span), f32),
            pltpu.VMEM((rows, qw), bf16),
            pltpu.VMEM((rows, 2 * kvw), bf16),
            pltpu.VMEM((doms, rows, 2 * kvw), bf16),
            pltpu.VMEM((tps - 1, rows, width), f32),
            pltpu.VMEM((tps - 1, rows, width), f32),
            pltpu.VMEM((tps, rows, HD), f32),
            pltpu.VMEM((doms, parts, HD), f32),
            pltpu.VMEM((doms, parts, HD), f32),
            pltpu.SemaphoreType.DMA((9,)),
            pltpu.SemaphoreType.DMA((3 * (tps - 1),)),
            pltpu.SemaphoreType.DMA((3 * (tps - 1),)),
            pltpu.SemaphoreType.DMA((3 * (doms - 1),)),
            pltpu.SemaphoreType.DMA((3 * (doms - 1),)),
            pltpu.SemaphoreType.DMA((32,)),
            pltpu.SemaphoreType.DMA((32,)),
        ],
        compiler_params=pltpu.CompilerParams(
            collective_id=0, has_side_effects=True, vmem_limit_bytes=56 << 20
        ),
        name="layer",
    )(
        activations.reshape(rows, width), norm_gain.reshape(1, -1), w_query, w_key,
        value_weight, w_output, cache_keys, cache_values, reward, twist_vec.reshape(1, -1),
        previous_log_weights.reshape(parts, 1), copy_counts.astype(f32).reshape(parts, 1),
        jnp.asarray(cosine), jnp.asarray(sine),
    )
    result = jax.ShapeDtypeStruct((parts, span + steps, kvw), bf16)
    new_k, new_v = pl.pallas_call(
        functools.partial(select_kernel, parts, steps),
        out_shape=(result, result),
        in_specs=[pl.BlockSpec(memory_space=pltpu.SMEM), vmem, hbm, hbm],
        out_specs=(vmem, vmem),
        scratch_shapes=[pltpu.SemaphoreType.DMA((2 * parts,))],
        name="select",
    )(anc[0], fresh_sel, all_k, all_v)
    return attn.reshape(steps, parts, width), new_k, new_v, out_lw[:, 0]


def solution(mesh):
    body = fused if mesh.shape["dom"] == 8 else local
    return jax.shard_map(
        body,
        mesh=mesh,
        in_specs=(
            P(None, "dom", "tp"),
            P(),
            P(None, "tp"),
            P(None, "tp"),
            P(None, "tp"),
            P("tp", None),
            P("dom", None, "tp"),
            P("dom", None, "tp"),
            P(None, "dom"),
            P(),
            P("tp"),
            P("dom"),
            P("dom"),
        ),
        out_specs=(P(None, "dom", "tp"), P("dom", None, "tp"), P("dom", None, "tp"), P("dom")),
        check_vma=False,
    )
```

```python
import functools

import jax
import jax.numpy as jnp
import numpy as np
from jax import lax
from jax.experimental import pallas as pl
from jax.experimental.pallas import tpu as pltpu
from jax.sharding import PartitionSpec as P

D = 4096
HD = 128


def rotate(tensor, positions):
    middle = tensor.shape[-1] // 2
    frequency = 500000.0 ** (-2.0 * jnp.arange(middle, dtype=jnp.float32) / tensor.shape[-1])
    angles = positions[:, None] * frequency[None, :]
    cosine = jnp.cos(angles)[:, None, None, :]
    sine_part = jnp.sin(angles)[:, None, None, :]
    lower_half = tensor[..., :middle]
    upper_half = tensor[..., middle:]
    return jnp.concatenate(
        [
            lower_half * cosine - upper_half * sine_part,
            upper_half * cosine + lower_half * sine_part,
        ],
        -1,
    )


def local(
    activations,
    norm_gain,
    w_query,
    w_key,
    value_weight,
    w_output,
    cache_keys,
    cache_values,
    tokens,
    twisting_table,
    twist_vec,
    previous_log_weights,
    copy_counts,
):
    step_count = activations.shape[0]
    particle_count = activations.shape[1]
    span_old = cache_keys.shape[1]
    dom_size = lax.axis_size("dom")
    kv_local = w_key.shape[1] // HD
    q_local = w_query.shape[1] // HD
    group_size = q_local // kv_local
    all_counts = lax.all_gather(copy_counts, "dom", axis=0, tiled=True)
    copy_ends = jnp.cumsum(all_counts)
    ranks = jnp.arange(particle_count, dtype=jnp.int32) * dom_size + lax.axis_index("dom")
    ancestor = jnp.sum((copy_ends[None, :] <= ranks[:, None]).astype(jnp.int32), 1)
    all_keys = lax.all_gather(cache_keys, "dom", axis=0, tiled=True)
    all_values = lax.all_gather(cache_values, "dom", axis=0, tiled=True)

    gathered = lax.all_gather(activations, "tp", axis=2, tiled=True)
    inputs = gathered.astype(jnp.float32)
    normed = (
        inputs * lax.rsqrt(jnp.mean(inputs * inputs, -1, keepdims=True) + 1e-05) * norm_gain
    ).astype(jnp.bfloat16)
    flat_rows = normed.reshape(step_count * particle_count, D)
    positions = (span_old + jnp.arange(step_count, dtype=jnp.int32)).astype(jnp.float32)
    queries = jnp.dot(flat_rows, w_query, preferred_element_type=jnp.float32).reshape(
        step_count, particle_count, q_local, HD
    )
    queries = rotate(queries, positions).astype(jnp.bfloat16)
    fresh_keys = jnp.dot(flat_rows, w_key, preferred_element_type=jnp.float32).reshape(
        step_count, particle_count, kv_local, HD
    )
    fresh_keys = (
        rotate(fresh_keys, positions)
        .astype(jnp.bfloat16)
        .reshape(step_count, particle_count, kv_local * HD)
    )
    fresh_values = jnp.dot(flat_rows, value_weight, preferred_element_type=jnp.float32).astype(
        jnp.bfloat16
    )
    fresh_values = fresh_values.reshape(step_count, particle_count, kv_local * HD)
    fresh_keys = jnp.transpose(fresh_keys, (1, 0, 2))
    fresh_values = jnp.transpose(fresh_values, (1, 0, 2))
    key_rows = jnp.concatenate([cache_keys, fresh_keys], 1)
    value_rows = jnp.concatenate([cache_values, fresh_values], 1)
    key_span = span_old + step_count
    query_heads = queries.reshape(step_count, particle_count, kv_local, group_size, HD)
    key_heads = key_rows.reshape(particle_count, key_span, kv_local, HD)
    value_heads = value_rows.reshape(particle_count, key_span, kv_local, HD)
    scores = (
        jnp.einsum("snkgd,nlkd->snkgl", query_heads, key_heads, preferred_element_type=jnp.float32)
        / HD**0.5
    )
    allowed = (
        jnp.arange(key_span, dtype=jnp.int32)[None, :]
        <= (span_old + jnp.arange(step_count, dtype=jnp.int32))[:, None]
    )
    allowed = allowed[:, None, None, None, :]
    masked = jnp.where(allowed, scores, -jnp.inf)
    highest = jnp.max(masked, -1, keepdims=True)
    exponent = jnp.exp(masked - highest)
    weights = (exponent / jnp.sum(exponent, -1, keepdims=True)).astype(jnp.bfloat16)
    context = jnp.einsum(
        "snkgl,nlkd->snkgd", weights, value_heads, preferred_element_type=jnp.float32
    ).astype(jnp.bfloat16)
    context = context.reshape(step_count * particle_count, q_local * HD)
    partial_value = jnp.dot(context, w_output, preferred_element_type=jnp.float32).reshape(
        step_count, particle_count, D
    )
    head_mix = lax.psum_scatter(partial_value, "tp", scatter_dimension=2, tiled=True)
    attn_out = head_mix.astype(jnp.bfloat16)
    summed = activations.astype(jnp.float32) + head_mix
    aligned, energy = lax.psum(
        (jnp.sum(summed * twist_vec, -1), jnp.sum(summed * summed, -1)), "tp"
    )
    twisting_score = aligned / jnp.sqrt(energy / D + 1e-06)
    token_reward = twisting_table[tokens].astype(jnp.float32)
    particle_log_weight = previous_log_weights + jnp.sum(token_reward + twisting_score, 0)
    largest = lax.pmax(jnp.max(particle_log_weight), "dom")
    mass_total = lax.psum(jnp.sum(jnp.exp(particle_log_weight - largest)), "dom")
    out_logw = particle_log_weight - (largest + jnp.log(mass_total))
    fresh = lax.all_gather(
        jnp.concatenate([fresh_keys, fresh_values], 2), "dom", axis=0, tiled=True
    )[ancestor]
    width = fresh_keys.shape[2]
    new_keys = jnp.concatenate([all_keys[ancestor], fresh[..., :width]], 1)
    new_values = jnp.concatenate([all_values[ancestor], fresh[..., width:]], 1)
    return (attn_out, new_keys, new_values, out_logw)


MESH = pl.DeviceIdType.MESH


def layer_kernel(
    steps, parts, doms, tps,
    act, gain, wq, wk, wv, wo, ck, cv, twist, aux, cosine, sine,
    attn_out, all_k, all_v, fresh_sel, out_lw, anc_out,
    act_all, wq_v, wk_v, wv_v, wo_v, ck_v, cv_v, qs, cx, sc1, ctx_b, fresh, fresh_all,
    rs_send, rs_recv, sc_all, lw_all, cnt_all,
    loc, tp_send, tp_recv, dom_send, dom_recv, blk_send, blk_recv,
):
    f32, bf16 = jnp.float32, jnp.bfloat16
    me_d = lax.axis_index("dom")
    me_t = lax.axis_index("tp")
    rows, width = act.shape
    half = parts // 2
    kvw = wk.shape[1]
    groups = kvw // HD
    per = wq.shape[1] // kvw
    pack = steps * per
    c = me_d % 2
    x = (me_d // 2) % 2
    y = me_d // 4
    sib = me_d + 1 - 2 * c
    xn = me_d + 2 - 4 * x
    yn = me_d + 4 - 8 * y
    dn = xn + 4 - 8 * y

    barrier = pltpu.get_barrier_semaphore()
    for k in range(1, tps):
        pl.semaphore_signal(
            barrier, inc=1, device_id=(me_d, (me_t + k) % tps), device_id_type=MESH
        )
    for k in range(1, doms):
        pl.semaphore_signal(
            barrier, inc=1, device_id=((me_d + k) % doms, me_t), device_id_type=MESH
        )

    def fetch(i, src, dst):
        copy = pltpu.make_async_copy(src, dst, loc.at[i])
        copy.start()
        return copy

    own_act = fetch(0, act, act_all.at[me_t])
    load_q = fetch(1, wq, wq_v)
    load_k = fetch(2, wk, wk_v)
    load_v = fetch(3, wv, wv_v)
    load_ck = fetch(4, ck, ck_v)
    load_cv = fetch(5, cv, cv_v)
    load_o = fetch(6, wo, wo_v)

    cnt_all[me_d] = jnp.broadcast_to(aux[:, 1:], cnt_all.shape[1:])
    pl.semaphore_wait(barrier, tps + doms - 2)

    def tp_push(base, k, src, dst):
        copy = pltpu.make_async_remote_copy(
            src_ref=src, dst_ref=dst, send_sem=tp_send.at[base + k - 1],
            recv_sem=tp_recv.at[base + k - 1],
            device_id=(me_d, (me_t + k) % tps), device_id_type=MESH,
        )
        copy.start()
        return copy

    def dom_push(base, k, src, dst):
        copy = pltpu.make_async_remote_copy(
            src_ref=src, dst_ref=dst, send_sem=dom_send.at[base + k - 1],
            recv_sem=dom_recv.at[base + k - 1],
            device_id=((me_d + k) % doms, me_t), device_id_type=MESH,
        )
        copy.start()
        return copy

    acts = [tp_push(0, k, act, act_all.at[me_t]) for k in range(1, tps)]

    def piece(kind, to, which, h, slot, own):
        dst = (all_k, all_v)[which].at[slot, pl.ds(h * half, half)]
        src = (ck, cv)[which].at[pl.ds(h * half, half)] if own else dst
        i = kind * 4 + h * 2 + which
        copy = pltpu.make_async_remote_copy(
            src_ref=src, dst_ref=dst, send_sem=blk_send.at[i], recv_sem=blk_recv.at[i],
            device_id=(to, me_t), device_id_type=MESH,
        )
        copy.start()
        return copy

    moves = {}
    for h, kind, to in ((0, 0, xn), (1, 1, yn), (1, 0, xn), (0, 1, yn)):
        for which in range(2):
            moves[kind, h, which] = piece(kind, to, which, h, me_d, True)
    cnts = [dom_push(0, k, cnt_all.at[me_d], cnt_all.at[me_d]) for k in range(1, doms)]
    for h in range(2):
        for which in range(2):
            moves[3, h, which] = piece(3, sib, which, h, me_d, True)

    own_act.wait()
    for copy in acts:
        copy.wait()
    square = jnp.zeros((rows, 1), f32)
    for t in range(tps):
        u = act_all[t].astype(f32)
        square = square + jnp.sum(u * u, -1, keepdims=True)
    inv = lax.rsqrt(square / (width * tps) + 1e-05)
    normed = []
    for t in range(tps):
        u = act_all[t].astype(f32)
        normed.append((u * inv * gain[:, t * width : (t + 1) * width]).astype(bf16))

    def project(w):
        total = None
        for t in range(tps):
            part = jnp.dot(
                normed[t], w[t * width : (t + 1) * width, :], preferred_element_type=f32
            )
            total = part if total is None else total + part
        return total

    cos_t, sin_t = cosine[...], sine[...]

    def turn(u):
        return u * cos_t + pltpu.roll(u, HD // 2, 1) * sin_t

    load_k.wait()
    load_v.wait()
    keys = project(wk_v)
    for g in range(groups):
        fresh[:, g * HD : (g + 1) * HD] = turn(keys[:, g * HD : (g + 1) * HD]).astype(bf16)
    fresh[:, kvw:] = project(wv_v).astype(bf16)
    fresh_all[me_d] = fresh[...]
    news = [dom_push(doms - 1, k, fresh, fresh_all.at[me_d]) for k in range(1, doms)]
    load_q.wait()
    query = project(wq_v)
    for h in range(groups * per):
        g, j = h // per, h % per
        turned = turn(query[:, h * HD : (h + 1) * HD])
        for s in range(steps):
            qs[g, :, s * per + j, :] = turned[s * parts : (s + 1) * parts]
    load_ck.wait()
    load_cv.wait()
    put_k = fetch(7, ck_v, all_k.at[me_d])
    put_v = fetch(8, cv_v, all_v.at[me_d])

    lines = parts * pack
    row = lax.broadcasted_iota(jnp.int32, (lines, rows), 0)
    col = lax.broadcasted_iota(jnp.int32, (lines, rows), 1)
    allowed = (row // pack == col % parts) & (col // parts <= (row % pack) // per)
    scale = HD**0.5
    for g in range(groups):
        lanes = slice(g * HD, (g + 1) * HD)
        qg = qs[g].reshape(lines, HD).astype(bf16)
        for n in range(parts):
            sc1[g, n * pack : (n + 1) * pack, :] = lax.dot_general(
                qg[n * pack : (n + 1) * pack], ck_v[n, :, lanes],
                (((1,), (1,)), ((), ())), preferred_element_type=f32,
            )
        near = lax.dot_general(
            qg, fresh[:, lanes], (((1,), (1,)), ((), ())), preferred_element_type=f32
        )
        near = jnp.where(allowed, near / scale, -jnp.inf)
        far = sc1[g] / scale
        top = jnp.maximum(
            jnp.max(far, -1, keepdims=True), jnp.max(near, -1, keepdims=True)
        )
        far = jnp.exp(far - top)
        near = jnp.exp(near - top)
        mass = jnp.sum(far, -1, keepdims=True) + jnp.sum(near, -1, keepdims=True)
        far = (far / mass).astype(bf16)
        near = (near / mass).astype(bf16)
        extra = jnp.dot(
            near, fresh[:, kvw + g * HD : kvw + (g + 1) * HD], preferred_element_type=f32
        )
        for n in range(parts):
            span = slice(n * pack, (n + 1) * pack)
            cx[g, n] = extra[span] + jnp.dot(
                far[span], cv_v[n, :, lanes], preferred_element_type=f32
            )
    for h in range(groups * per):
        g, j = h // per, h % per
        for s in range(steps):
            ctx_b[s * parts : (s + 1) * parts, h * HD : (h + 1) * HD] = cx[
                g, :, s * per + j, :
            ].astype(bf16)
    load_o.wait()

    def mix(p):
        return jnp.dot(
            ctx_b[...], wo_v[:, pl.ds(pl.multiple_of(p * width, HD), width)],
            preferred_element_type=f32,
        )

    sums = []
    for k in range(1, tps):
        rs_send[k - 1] = mix((me_t + k) % tps)
        sums.append(tp_push(tps - 1, k, rs_send.at[k - 1], rs_recv.at[k - 1]))
    head = mix(me_t)

    def done(kind, h):
        for which in range(2):
            moves[kind, h, which].wait_recv()

    def relay(kind, to, h, slot):
        for which in range(2):
            moves[kind, h, which] = piece(kind, to, which, h, slot, False)

    done(0, 0)
    relay(2, yn, 0, xn)
    relay(4, sib, 0, xn)
    done(1, 1)
    relay(6, xn, 1, yn)
    relay(5, sib, 1, yn)
    for k in range(1, tps):
        sums[k - 1].wait()
        head = head + rs_recv[k - 1]
    attn_out[...] = head.astype(bf16)
    summed = act_all[me_t].astype(f32) + head
    along = jnp.sum(summed * twist[...], -1, keepdims=True)
    energy = jnp.sum(summed * summed, -1, keepdims=True)
    lane = lax.broadcasted_iota(jnp.int32, (rows, HD), 1)
    sc_all[me_t] = jnp.where(lane < HD // 2, along, energy)
    scores = [
        tp_push(2 * (tps - 1), k, sc_all.at[me_t], sc_all.at[me_t]) for k in range(1, tps)
    ]
    for copy in scores:
        copy.wait()
    both = sc_all[0]
    for t in range(1, tps):
        both = both + sc_all[t]
    score = both[:, :1] / jnp.sqrt(both[:, HD - 1 :] / (width * tps) + 1e-06)
    total = score[:parts]
    for s in range(1, steps):
        total = total + score[s * parts : (s + 1) * parts]
    mine = jnp.broadcast_to(aux[:, :1] + total, (parts, HD))
    lw_all[me_d] = mine
    lws = [
        dom_push(2 * (doms - 1), k, lw_all.at[me_d], lw_all.at[me_d]) for k in range(1, doms)
    ]

    done(0, 1)
    relay(4, sib, 1, xn)
    done(1, 0)
    relay(5, sib, 0, yn)

    for copy in cnts:
        copy.wait()
    for copy in news:
        copy.wait()
    whole = parts * doms
    number = cnt_all[...].reshape(whole, HD).astype(bf16)
    lower = lax.broadcasted_iota(jnp.int32, (whole, whole), 0)
    upper = lax.broadcasted_iota(jnp.int32, (whole, whole), 1)
    ends = jnp.dot(
        (upper <= lower).astype(f32).astype(bf16), number, preferred_element_type=f32
    )
    slot = lax.broadcasted_iota(jnp.int32, (whole, HD), 1)

    def ancestor(place):
        rank = (place * doms + me_d).astype(f32)
        return jnp.sum((ends <= rank).astype(f32), 0, keepdims=True).astype(jnp.int32)

    anc_out[...] = jnp.broadcast_to(ancestor(slot), anc_out.shape)
    lanes = lax.broadcasted_iota(jnp.int32, (1, HD), 1)
    wide = ancestor(slot // 8)
    target = (wide // parts) * rows + (lanes % 8) * parts + wide % parts
    target = jnp.where(lanes % 8 < steps, target, -1)
    index = lax.broadcasted_iota(jnp.int32, (doms * rows, HD), 0)
    pick = (index == target).astype(f32).astype(bf16)
    fresh_sel[...] = lax.dot_general(
        pick, fresh_all[...].reshape(doms * rows, 2 * kvw),
        (((0,), (0,)), ((), ())), preferred_element_type=f32,
    ).astype(bf16)

    for copy in lws:
        copy.wait()
    largest = jnp.max(lw_all[...], (0, 1), keepdims=True)[0]
    mass = jnp.sum(jnp.exp(lw_all[...] - largest[None]), (0, 1), keepdims=True)[0]
    out_lw[...] = mine - (largest + jnp.log(mass))

    done(2, 0)
    relay_d0 = [piece(7, sib, which, 0, dn, False) for which in range(2)]
    done(6, 1)
    relay_d1 = [piece(7, sib, which, 1, dn, False) for which in range(2)]
    for kind in (3, 4, 5):
        for h in range(2):
            done(kind, h)
    for copy in moves.values():
        copy.wait_send()
    for copy in relay_d0 + relay_d1:
        copy.wait()
    put_k.wait()
    put_v.wait()


def select_kernel(parts, steps, anc, fresh_sel, all_k, all_v, new_k, new_v, sem):
    span = all_k.shape[2]
    width = all_k.shape[3]
    copies = []
    for i in range(parts):
        a = anc[0, i]
        d, n = a // parts, a % parts
        for which, (src, dst) in enumerate(((all_k, new_k), (all_v, new_v))):
            copy = pltpu.make_async_copy(
                src.at[d, n], dst.at[i, pl.ds(0, span)], sem.at[2 * i + which]
            )
            copy.start()
            copies.append(copy)
    for i in range(parts):
        new_k[i, span:, :] = fresh_sel[i * 8 : i * 8 + steps, :width]
        new_v[i, span:, :] = fresh_sel[i * 8 : i * 8 + steps, width:]
    for copy in copies:
        copy.wait()


def fused(
    activations, norm_gain, w_query, w_key, value_weight, w_output, cache_keys, cache_values,
    tokens, twisting_table, twist_vec, previous_log_weights, copy_counts,
):
    f32, bf16 = jnp.float32, jnp.bfloat16
    steps, parts, width = activations.shape
    rows = steps * parts
    span = cache_keys.shape[1]
    kvw = w_key.shape[1]
    qw = w_query.shape[1]
    groups = kvw // HD
    pack = steps * (qw // kvw)
    doms = lax.axis_size("dom")
    tps = lax.axis_size("tp")
    middle = HD // 2
    angles = (span + np.arange(rows) // parts)[:, None] * (
        500000.0 ** (-2.0 * np.arange(middle) / HD)
    )
    cosine = np.concatenate([np.cos(angles)] * 2, 1).astype(np.float32)
    sine = np.concatenate([-np.sin(angles), np.sin(angles)], 1).astype(np.float32)
    reward = jnp.sum(twisting_table[tokens].astype(f32), 0)
    aux = jnp.stack([previous_log_weights + reward, copy_counts.astype(f32)], 1)
    vmem = pl.BlockSpec(memory_space=pltpu.VMEM)
    hbm = pl.BlockSpec(memory_space=pl.ANY)
    block = jax.ShapeDtypeStruct((doms,) + cache_keys.shape, bf16)
    attn, all_k, all_v, fresh_sel, out_lw, anc = pl.pallas_call(
        functools.partial(layer_kernel, steps, parts, doms, tps),
        out_shape=(
            jax.ShapeDtypeStruct((rows, width), bf16), block, block,
            jax.ShapeDtypeStruct((HD, 2 * kvw), bf16),
            jax.ShapeDtypeStruct((parts, HD), f32),
            jax.ShapeDtypeStruct((8, HD), jnp.int32),
        ),
        in_specs=[hbm, vmem] + [hbm] * 6 + [vmem] * 4,
        out_specs=(vmem, hbm, hbm, vmem, vmem, vmem),
        scratch_shapes=[
            pltpu.VMEM((tps, rows, width), bf16),
            pltpu.VMEM(w_query.shape, bf16),
            pltpu.VMEM(w_key.shape, bf16),
            pltpu.VMEM(value_weight.shape, bf16),
            pltpu.VMEM(w_output.shape, bf16),
            pltpu.VMEM(cache_keys.shape, bf16),
            pltpu.VMEM(cache_values.shape, bf16),
            pltpu.VMEM((groups, parts, pack, HD), f32),
            pltpu.VMEM((groups, parts, pack, HD), f32),
            pltpu.VMEM((groups, parts * pack, span), f32),
            pltpu.VMEM((rows, qw), bf16),
            pltpu.VMEM((rows, 2 * kvw), bf16),
            pltpu.VMEM((doms, rows, 2 * kvw), bf16),
            pltpu.VMEM((tps - 1, rows, width), f32),
            pltpu.VMEM((tps - 1, rows, width), f32),
            pltpu.VMEM((tps, rows, HD), f32),
            pltpu.VMEM((doms, parts, HD), f32),
            pltpu.VMEM((doms, parts, HD), f32),
            pltpu.SemaphoreType.DMA((9,)),
            pltpu.SemaphoreType.DMA((3 * (tps - 1),)),
            pltpu.SemaphoreType.DMA((3 * (tps - 1),)),
            pltpu.SemaphoreType.DMA((3 * (doms - 1),)),
            pltpu.SemaphoreType.DMA((3 * (doms - 1),)),
            pltpu.SemaphoreType.DMA((32,)),
            pltpu.SemaphoreType.DMA((32,)),
        ],
        compiler_params=pltpu.CompilerParams(
            collective_id=0, has_side_effects=True, vmem_limit_bytes=56 << 20
        ),
        name="layer",
    )(
        activations.reshape(rows, width), norm_gain.reshape(1, -1), w_query, w_key,
        value_weight, w_output, cache_keys, cache_values, twist_vec.reshape(1, -1), aux,
        jnp.asarray(cosine), jnp.asarray(sine),
    )
    result = jax.ShapeDtypeStruct((parts, span + steps, kvw), bf16)
    new_k, new_v = pl.pallas_call(
        functools.partial(select_kernel, parts, steps),
        out_shape=(result, result),
        in_specs=[pl.BlockSpec(memory_space=pltpu.SMEM), vmem, hbm, hbm],
        out_specs=(vmem, vmem),
        scratch_shapes=[pltpu.SemaphoreType.DMA((2 * parts,))],
        name="select",
    )(anc, fresh_sel, all_k, all_v)
    return attn.reshape(steps, parts, width), new_k, new_v, out_lw[:, 0]


def solution(mesh):
    body = fused if mesh.shape["dom"] == 8 else local
    return jax.shard_map(
        body,
        mesh=mesh,
        in_specs=(
            P(None, "dom", "tp"),
            P(),
            P(None, "tp"),
            P(None, "tp"),
            P(None, "tp"),
            P("tp", None),
            P("dom", None, "tp"),
            P("dom", None, "tp"),
            P(None, "dom"),
            P(),
            P("tp"),
            P("dom"),
            P("dom"),
        ),
        out_specs=(P(None, "dom", "tp"), P("dom", None, "tp"), P("dom", None, "tp"), P("dom")),
        check_vma=False,
    )
```
